8 devices in a mesh: rep: 1 (over z), dp: 8 (over x, y, core).
Axes of the slice: x: 2, y: 2, z: 1, core: 2. Of those that a mesh axis runs over, the one named last changes fastest.
Arguments:
- a: bfloat16 [8, 4, 4096, 1024], P(('rep', 'dp'))
- g: bfloat16 [8, 4, 4096, 3200], P(('rep', 'dp'))
Outputs:
- output: bfloat16 [4, 1024, 3200], P('rep')
All inputs are finite; a program needn't handle non-finite values.
Results may differ from the reference program's by a relative error of at most 0.012.
Values are sent between devices in bfloat16 or wider.
A program may use at most 2 GiB of HBM per device.

```python
import jax
import jax.numpy as jnp
from jax import lax

DEVICES = 8
MATRICES = 4
TOKENS = 4096
D = 1024
FF = 3200


def setup_inputs(seed: int = 0, part: int = 0) -> dict:
    ka, kg, ks = (jax.random.fold_in(k, part) for k in jax.random.split(jax.random.key(seed), 3))
    size = 2.0 ** jax.random.uniform(ks, (DEVICES, MATRICES, 1, 1), jnp.float32, -1.0, 1.0)
    a = jax.random.normal(ka, (DEVICES, MATRICES, TOKENS, D), jnp.float32)
    g = size * jax.random.normal(kg, (DEVICES, MATRICES, TOKENS, FF), jnp.float32) * (DEVICES * TOKENS) ** -0.5
    return {"a": a.astype(jnp.bfloat16), "g": g.astype(jnp.bfloat16)}


def reference(a, g):
    def take(so_far, one):
        return so_far + jnp.einsum("ntd,ntf->ndf", *one, preferred_element_type=jnp.float32), None

    return lax.scan(take, jnp.zeros((MATRICES, D, FF), jnp.float32), (a, g))[0].astype(jnp.bfloat16)
```

```python
import functools

import jax
import jax.numpy as jnp
from jax import lax
from jax.experimental import pallas as pl
from jax.experimental.pallas import tpu as pltpu
from jax.sharding import PartitionSpec as P

MESH = pl.DeviceIdType.MESH
ROWS, COLS = 512, 640
RING = 4
GATHER_FROM, GATHER_EVERY = 4, 2


def kernel(dims, a, g, out, a_v, g_v, half_send, half_own, half_recv, one_send, one_own, one_recv, two_send, two_own,
           two_recv, final, sem_a, sem_g, sem_hs, sem_hr, sem_1s, sem_1r, sem_2s, sem_2r, sem_fin, sem_3s, sem_3r,
           sem_4s, sem_4r, sem_5s, sem_5r, sem_6s, sem_6r):
    mats, tokens, d, ff = dims
    row_blocks, col_blocks = d // ROWS, ff // COLS
    steps = mats * row_blocks * col_blocks
    half, quarter, eighth = ROWS // 2, ROWS // 4, ROWS // 8

    me = lax.axis_index("dp")
    core, y, x = me % 2, (me // 2) % 2, me // 4
    mate = me + 1 - 2 * core
    first_bit = x * (1 - core) + y * core
    second_bit = y * (1 - core) + x * core
    first = me + (1 - 2 * first_bit) * (4 - 2 * core)
    second = me + (1 - 2 * second_bit) * (2 + 2 * core)

    def send(src, dst, send_sem, recv_sem, to):
        return pltpu.make_async_remote_copy(src, dst, send_sem, recv_sem, device_id={"dp": to}, device_id_type=MESH)

    barrier = pltpu.get_barrier_semaphore()
    for to in (mate, first, second):
        pl.semaphore_signal(barrier, 1, device_id={"dp": to}, device_id_type=MESH)

    def place(k):
        n = k // (row_blocks * col_blocks)
        rest = k % (row_blocks * col_blocks)
        return n, rest // row_blocks, rest % row_blocks

    def load_a(n, r):
        cols = pl.ds(pl.multiple_of(r * ROWS, ROWS), ROWS)
        return pltpu.make_async_copy(a.at[0, n, :, cols], a_v.at[n % 2, :, cols], sem_a.at[n % 2, r])

    def load_g(i):
        n, c = i // col_blocks, i % col_blocks
        cols = pl.ds(pl.multiple_of(c * COLS, 128), COLS)
        return pltpu.make_async_copy(g.at[0, n, :, cols], g_v.at[i % 2], sem_g.at[i % 2])

    def rows_of(k, start, size):
        n, c, r = place(k)
        return out.at[n, pl.ds(pl.multiple_of(r * ROWS + start, eighth), size), pl.ds(pl.multiple_of(c * COLS, 128), COLS)]

    own_half = core * half
    here = own_half + first_bit * quarter + second_bit * eighth
    there = own_half + first_bit * quarter + (1 - second_bit) * eighth

    def swap(k):
        return send(half_send.at[k % 2], half_recv.at[k], sem_hs.at[k % 2], sem_hr.at[k], mate)

    def exchange_one(k):
        return send(one_send.at[k % RING], one_recv.at[k], sem_1s.at[k % RING], sem_1r.at[k], first)

    def exchange_two(k):
        return send(two_send.at[k % RING], two_recv.at[k], sem_2s.at[k % RING], sem_2r.at[k], second)

    def keep(k):
        return pltpu.make_async_copy(final.at[k], rows_of(k, here, eighth), sem_fin.at[k])

    def gather_second(k):
        return send(final.at[k], rows_of(k, here, eighth), sem_3s.at[k], sem_3r.at[k], second)

    def gather_first(k):
        return send(final.at[k], rows_of(k, here, eighth), sem_4s.at[k], sem_4r.at[k], first)

    def relay(k):
        return send(rows_of(k, there, eighth), rows_of(k, there, eighth), sem_5s.at[k], sem_5r.at[k], first)

    def hand_over(k):
        return send(rows_of(k, own_half, half), rows_of(k, own_half, half), sem_6s.at[k], sem_6r.at[k], mate)

    def product(k, start):
        n, c, r = place(k)
        cols = pl.ds(pl.multiple_of(r * ROWS + start, half), half)
        return lax.dot_general(
            a_v[n % 2, :, cols], g_v[(k // row_blocks) % 2], (((0,), (0,)), ((), ())), preferred_element_type=jnp.float32
        )

    def part(ref, slot, bit, size):
        return ref[slot, pl.ds(pl.multiple_of(bit * size, size), size), :]

    def reduce_cores(k):
        swap(k).wait_recv()

        @pl.when(k >= RING)
        def _():
            exchange_one(k - RING).wait_send()

        def total(bit):
            return part(half_own, k % 2, bit, quarter) + part(half_recv, k, bit, quarter).astype(jnp.float32)

        one_send[k % RING] = total(1 - first_bit).astype(jnp.bfloat16)
        one_own[k % 2] = total(first_bit)
        exchange_one(k).start()

    def reduce_first(k):
        exchange_one(k).wait_recv()

        @pl.when(k >= RING)
        def _():
            exchange_two(k - RING).wait_send()

        def total(bit):
            return part(one_own, k % 2, bit, eighth) + part(one_recv, k, bit, eighth).astype(jnp.float32)

        two_send[k % RING] = total(1 - second_bit).astype(jnp.bfloat16)
        two_own[k % 2] = total(second_bit)
        exchange_two(k).start()

    def reduce_second(k):
        exchange_two(k).wait_recv()
        final[k] = (two_own[k % 2] + two_recv[k].astype(jnp.float32)).astype(jnp.bfloat16)
        keep(k).start()

    def gather(k):
        gather_second(k).start()
        gather_first(k).start()

    def pass_on(k):
        gather_second(k).wait_recv()
        relay(k).start()

    def finish(k):
        keep(k).wait()
        gather_first(k).wait_recv()
        relay(k).wait_recv()
        hand_over(k).start()

    load_a(0, 0).start()
    load_g(0).start()
    for r in range(1, row_blocks):
        load_a(0, r).start()
    pl.semaphore_wait(barrier, 3)

    def step(k, carry):
        n, c, r = place(k)

        @pl.when(r == 0)
        def _():
            load_g(k // row_blocks).wait()

            @pl.when(k + row_blocks < steps)
            def _():
                load_g(k // row_blocks + 1).start()

        @pl.when(c == 0)
        def _():
            load_a(n, r).wait()

            @pl.when(n + 1 < mats)
            def _():
                load_a(n + 1, r).start()

        @pl.when(k >= 2)
        def _():
            swap(k - 2).wait_send()

        half_send[k % 2] = product(k, (1 - core) * half).astype(jnp.bfloat16)
        swap(k).start()
        half_own[k % 2] = product(k, own_half)
        reduce_cores(k)

        @pl.when(k >= 1)
        def _():
            reduce_first(k - 1)

        @pl.when(k >= 2)
        def _():
            reduce_second(k - 2)

        @pl.when((k >= GATHER_FROM) & ((k - GATHER_FROM) % GATHER_EVERY == 0))
        def _():
            i = (k - GATHER_FROM) // GATHER_EVERY
            gather(i)

            @pl.when(i >= 2)
            def _():
                pass_on(i - 2)

            @pl.when(i >= 4)
            def _():
                finish(i - 4)

        return carry

    lax.fori_loop(0, steps, step, 0)
    reduce_first(steps - 1)
    reduce_second(steps - 2)
    reduce_second(steps - 1)

    started = (steps - 1 - GATHER_FROM) // GATHER_EVERY + 1

    def loop(low, high, f):
        def body(k, carry):
            f(k)
            return carry

        lax.fori_loop(low, high, body, 0)

    loop(started, steps, gather)
    loop(started - 2, steps, pass_on)
    loop(started - 4, steps, finish)

    def drain(k):
        gather_second(k).wait_send()
        gather_first(k).wait_send()
        relay(k).wait_send()
        hand_over(k).wait()

    loop(0, steps, drain)
    for k in range(steps - 2, steps):
        swap(k).wait_send()
    for k in range(steps - RING, steps):
        exchange_one(k).wait_send()
        exchange_two(k).wait_send()


def solution(mesh):
    def step(a, g):
        _, mats, tokens, d = a.shape
        ff = g.shape[-1]
        steps = mats * (d // ROWS) * (ff // COLS)
        half, quarter, eighth = ROWS // 2, ROWS // 4, ROWS // 8
        bf16, f32 = jnp.bfloat16, jnp.float32
        dma = pltpu.SemaphoreType.DMA
        return pl.pallas_call(
            functools.partial(kernel, (mats, tokens, d, ff)),
            out_shape=jax.ShapeDtypeStruct((mats, d, ff), bf16),
            in_specs=[pl.BlockSpec(memory_space=pl.ANY)] * 2,
            out_specs=pl.BlockSpec(memory_space=pl.ANY),
            scratch_shapes=[
                pltpu.VMEM((2, tokens, d), bf16),
                pltpu.VMEM((2, tokens, COLS), bf16),
                pltpu.VMEM((2, half, COLS), bf16),
                pltpu.VMEM((2, half, COLS), f32),
                pltpu.VMEM((steps, half, COLS), bf16),
                pltpu.VMEM((RING, quarter, COLS), bf16),
                pltpu.VMEM((2, quarter, COLS), f32),
                pltpu.VMEM((steps, quarter, COLS), bf16),
                pltpu.VMEM((RING, eighth, COLS), bf16),
                pltpu.VMEM((2, eighth, COLS), f32),
                pltpu.VMEM((steps, eighth, COLS), bf16),
                pltpu.VMEM((steps, eighth, COLS), bf16),
                dma((2, d // ROWS)),
                dma((2,)),
                dma((2,)),
                dma((steps,)),
                dma((RING,)),
                dma((steps,)),
                dma((RING,)),
                dma((steps,)),
            ]
            + [dma((steps,))] * 9,
            compiler_params=pltpu.CompilerParams(
                collective_id=0, has_side_effects=True, vmem_limit_bytes=63 * 2**20
            ),
        )(a, g)

    return jax.shard_map(
        step,
        mesh=mesh,
        in_specs=(P(("rep", "dp")), P(("rep", "dp"))),
        out_specs=P("rep"),
        check_vma=False,
    )
```

```python
import functools

import jax
import jax.numpy as jnp
from jax import lax
from jax.experimental import pallas as pl
from jax.experimental.pallas import tpu as pltpu
from jax.sharding import PartitionSpec as P

MESH = pl.DeviceIdType.MESH
ROWS, COLS = 512, 640
VMEM_LIMIT = 63 * 2**20
LAG_ONE, LAG_TWO = 2, 4
RING_ONE, RING_TWO = 2 * LAG_ONE + 2, 2 * (LAG_TWO - LAG_ONE) + 2
OWN_ONE, OWN_TWO = LAG_ONE + 1, LAG_TWO - LAG_ONE + 1
GATHER_FROM, GATHER_SKIP = LAG_TWO, 6
PASS_LAG, FINISH_LAG = 2, 4
TAIL = 2


def kernel(dims, a, g, out, a_v, g_v, half_send, half_own, half_recv, one_send, one_own, one_recv, two_send, two_own,
           two_recv, final, sem_a, sem_g, sem_hs, sem_hr, sem_1s, sem_1r, sem_2s, sem_2r, sem_fin, sem_3s, sem_3r,
           sem_4s, sem_4r, sem_5s, sem_5r, sem_6s, sem_6r):
    mats, tokens, d, ff = dims
    row_blocks, col_blocks = d // ROWS, ff // COLS
    steps = mats * row_blocks * col_blocks
    half, quarter, eighth = ROWS // 2, ROWS // 4, ROWS // 8

    me = lax.axis_index("dp")
    core, y, x = me % 2, (me // 2) % 2, me // 4
    mate = me + 1 - 2 * core
    first_bit = x * (1 - core) + y * core
    second_bit = y * (1 - core) + x * core
    first = me + (1 - 2 * first_bit) * (4 - 2 * core)
    second = me + (1 - 2 * second_bit) * (2 + 2 * core)

    def send(src, dst, send_sem, recv_sem, to):
        return pltpu.make_async_remote_copy(src, dst, send_sem, recv_sem, device_id={"dp": to}, device_id_type=MESH)

    barrier = pltpu.get_barrier_semaphore()
    for to in (mate, first, second):
        pl.semaphore_signal(barrier, 1, device_id={"dp": to}, device_id_type=MESH)

    def place(k):
        n = k // (row_blocks * col_blocks)
        rest = k % (row_blocks * col_blocks)
        return n, rest // row_blocks, rest % row_blocks

    def load_a(n, r):
        cols = pl.ds(pl.multiple_of(r * ROWS, ROWS), ROWS)
        return pltpu.make_async_copy(a.at[0, n, :, cols], a_v.at[n % 2, :, cols], sem_a.at[n % 2, r])

    def load_g(i):
        n, c = i // col_blocks, i % col_blocks
        cols = pl.ds(pl.multiple_of(c * COLS, 128), COLS)
        return pltpu.make_async_copy(g.at[0, n, :, cols], g_v.at[i % 2], sem_g.at[i % 2])

    def index(k, start, size):
        n, c, r = place(k)
        return n, pl.ds(pl.multiple_of(r * ROWS + start, eighth), size), pl.ds(pl.multiple_of(c * COLS, 128), COLS)

    def rows_of(k, start, size):
        return out.at[index(k, start, size)]

    own_half = core * half
    here = own_half + first_bit * quarter + second_bit * eighth
    there = own_half + first_bit * quarter + (1 - second_bit) * eighth

    def swap(k):
        return send(half_send.at[k % 2], half_recv.at[k % 2], sem_hs.at[k % 2], sem_hr.at[k % 2], mate)

    def exchange_one(k):
        return send(one_send.at[k % RING_ONE], one_recv.at[k % RING_ONE], sem_1s.at[k % RING_ONE], sem_1r.at[k % RING_ONE], first)

    def exchange_two(k):
        return send(two_send.at[k % RING_TWO], two_recv.at[k % RING_TWO], sem_2s.at[k % RING_TWO], sem_2r.at[k % RING_TWO], second)

    def keep(k):
        return pltpu.make_async_copy(final.at[k], rows_of(k, here, eighth), sem_fin.at[k])

    def gather_second(k):
        return send(final.at[k], rows_of(k, here, eighth), sem_3s.at[k], sem_3r.at[k], second)

    def gather_first(k):
        return send(final.at[k], rows_of(k, here, eighth), sem_4s.at[k], sem_4r.at[k], first)

    def relay(k):
        return send(rows_of(k, there, eighth), rows_of(k, there, eighth), sem_5s.at[k], sem_5r.at[k], first)

    def hand_over(k):
        return send(rows_of(k, own_half, half), rows_of(k, own_half, half), sem_6s.at[k], sem_6r.at[k], mate)

    def product(k, start):
        n, c, r = place(k)
        cols = pl.ds(pl.multiple_of(r * ROWS + start, half), half)
        return lax.dot_general(
            a_v[n % 2, :, cols], g_v[(k // row_blocks) % 2], (((0,), (0,)), ((), ())), preferred_element_type=jnp.float32
        )

    def part(ref, slot, bit, size):
        return ref[slot, pl.ds(pl.multiple_of(bit * size, size), size), :]

    def reduce_cores(k):
        swap(k).wait_recv()

        @pl.when(k >= RING_ONE)
        def _():
            exchange_one(k - RING_ONE).wait_send()

        def total(bit):
            return part(half_own, k % 2, bit, quarter) + part(half_recv, k % 2, bit, quarter).astype(jnp.float32)

        one_send[k % RING_ONE] = total(1 - first_bit).astype(jnp.bfloat16)
        one_own[k % OWN_ONE] = total(first_bit)
        exchange_one(k).start()

    def reduce_first(k):
        exchange_one(k).wait_recv()

        @pl.when(k >= RING_TWO)
        def _():
            exchange_two(k - RING_TWO).wait_send()

        def total(bit):
            return part(one_own, k % OWN_ONE, bit, eighth) + part(one_recv, k % RING_ONE, bit, eighth).astype(jnp.float32)

        two_send[k % RING_TWO] = total(1 - second_bit).astype(jnp.bfloat16)
        two_own[k % OWN_TWO] = total(second_bit)
        exchange_two(k).start()

    def reduce_second(k):
        exchange_two(k).wait_recv()
        final[k] = (two_own[k % OWN_TWO] + two_recv[k % RING_TWO].astype(jnp.float32)).astype(jnp.bfloat16)
        keep(k).start()

    def gather(k):
        gather_second(k).start()
        gather_first(k).start()

    def pass_on(k):
        gather_second(k).wait_recv()
        relay(k).start()

    def finish(k):
        keep(k).wait()
        gather_first(k).wait_recv()
        relay(k).wait_recv()
        hand_over(k).start()

    load_a(0, 0).start()
    load_g(0).start()
    for r in range(1, row_blocks):
        load_a(0, r).start()
    pl.semaphore_wait(barrier, 3)

    def step(k, carry):
        n, c, r = place(k)

        @pl.when(r == 0)
        def _():
            load_g(k // row_blocks).wait()

            @pl.when(k + row_blocks < steps)
            def _():
                load_g(k // row_blocks + 1).start()

        @pl.when(c == 0)
        def _():
            load_a(n, r).wait()

            @pl.when(n + 1 < mats)
            def _():
                load_a(n + 1, r).start()

        @pl.when(k >= 2)
        def _():
            swap(k - 2).wait_send()

        half_send[k % 2] = product(k, (1 - core) * half).astype(jnp.bfloat16)
        swap(k).start()
        half_own[k % 2] = product(k, own_half)
        reduce_cores(k)

        @pl.when(k >= LAG_ONE)
        def _():
            reduce_first(k - LAG_ONE)

        @pl.when(k >= LAG_TWO)
        def _():
            reduce_second(k - LAG_TWO)

        since = k - GATHER_FROM

        @pl.when((since >= 0) & (since % GATHER_SKIP != GATHER_SKIP - 1))
        def _():
            i = since - since // GATHER_SKIP
            gather(i)

            @pl.when(i >= PASS_LAG)
            def _():
                pass_on(i - PASS_LAG)

            @pl.when(i >= FINISH_LAG)
            def _():
                finish(i - FINISH_LAG)

        return carry

    lax.fori_loop(0, steps, step, 0)
    since = steps - GATHER_FROM
    started = since - since // GATHER_SKIP

    def loop(low, high, f):
        def body(k, carry):
            f(k)
            return carry

        lax.fori_loop(low, high, body, 0)

    for k in range(steps, steps + LAG_TWO):
        if k - LAG_ONE < steps:
            reduce_first(k - LAG_ONE)
        reduce_second(k - LAG_TWO)
        ready = min(started + TAIL, k - LAG_TWO + 1) if k + 1 < steps + LAG_TWO else steps
        loop(started, ready, gather)
        started = max(started, ready)
    loop(since - since // GATHER_SKIP - PASS_LAG, steps, pass_on)
    loop(since - since // GATHER_SKIP - FINISH_LAG, steps, finish)

    def drain(k):
        gather_second(k).wait_send()
        gather_first(k).wait_send()
        relay(k).wait_send()
        hand_over(k).wait()

    loop(0, steps, drain)
    for k in range(steps - 2, steps):
        swap(k).wait_send()
    for k in range(steps - RING_ONE, steps):
        exchange_one(k).wait_send()
    for k in range(steps - RING_TWO, steps):
        exchange_two(k).wait_send()


def solution(mesh):
    def step(a, g):
        _, mats, tokens, d = a.shape
        ff = g.shape[-1]
        steps = mats * (d // ROWS) * (ff // COLS)
        half, quarter, eighth = ROWS // 2, ROWS // 4, ROWS // 8
        bf16, f32 = jnp.bfloat16, jnp.float32
        dma = pltpu.SemaphoreType.DMA
        return pl.pallas_call(
            functools.partial(kernel, (mats, tokens, d, ff)),
            out_shape=jax.ShapeDtypeStruct((mats, d, ff), bf16),
            in_specs=[pl.BlockSpec(memory_space=pl.ANY)] * 2,
            out_specs=pl.BlockSpec(memory_space=pl.ANY),
            scratch_shapes=[
                pltpu.VMEM((2, tokens, d), bf16),
                pltpu.VMEM((2, tokens, COLS), bf16),
                pltpu.VMEM((2, half, COLS), bf16),
                pltpu.VMEM((2, half, COLS), f32),
                pltpu.VMEM((2, half, COLS), bf16),
                pltpu.VMEM((RING_ONE, quarter, COLS), bf16),
                pltpu.VMEM((OWN_ONE, quarter, COLS), f32),
                pltpu.VMEM((RING_ONE, quarter, COLS), bf16),
                pltpu.VMEM((RING_TWO, eighth, COLS), bf16),
                pltpu.VMEM((OWN_TWO, eighth, COLS), f32),
                pltpu.VMEM((RING_TWO, eighth, COLS), bf16),
                pltpu.VMEM((steps, eighth, COLS), bf16),
                dma((2, d // ROWS)),
                dma((2,)),
                dma((2,)),
                dma((2,)),
                dma((RING_ONE,)),
                dma((RING_ONE,)),
                dma((RING_TWO,)),
                dma((RING_TWO,)),
            ]
            + [dma((steps,))] * 9,
            compiler_params=pltpu.CompilerParams(
                collective_id=0, has_side_effects=True, vmem_limit_bytes=VMEM_LIMIT
            ),
        )(a, g)

    return jax.shard_map(
        step,
        mesh=mesh,
        in_specs=(P(("rep", "dp")), P(("rep", "dp"))),
        out_specs=P("rep"),
        check_vma=False,
    )
```

```python
import functools

import jax
import jax.numpy as jnp
from jax import lax
from jax.experimental import pallas as pl
from jax.experimental.pallas import tpu as pltpu
from jax.sharding import PartitionSpec as P

MESH = pl.DeviceIdType.MESH
ROWS, COLS = 512, 640
VMEM_LIMIT = 63 * 2**20
LAG_ONE, LAG_TWO = 2, 4
RING_ONE, RING_TWO = 2 * LAG_ONE + 2, 2 * (LAG_TWO - LAG_ONE) + 2
OWN_ONE, OWN_TWO = LAG_ONE + 1, LAG_TWO - LAG_ONE + 1
GATHER_FROM, GATHER_SKIP = LAG_TWO, 6
PASS_LAG, FINISH_LAG = 2, 4
AFTER = 20
COPY_ROWS, COPY_SLOTS = 256, 6

TAIL = 2


def position(me):
    core, y, x = me % 2, (me // 2) % 2, me // 4
    return core, x * (1 - core) + y * core, y * (1 - core) + x * core


def place(dims, k):
    mats, tokens, d, ff = dims
    row_blocks, col_blocks = d // ROWS, ff // COLS
    rest = k % (row_blocks * col_blocks)
    return k // (row_blocks * col_blocks), rest // row_blocks, rest % row_blocks


def index(dims, k, start, size):
    n, c, r = place(dims, k)
    return n, pl.ds(pl.multiple_of(r * ROWS + start, size), size), pl.ds(pl.multiple_of(c * COLS, 128), COLS)


def kernel(dims, a, g, out, later, a_v, g_v, half_send, half_own, half_recv, one_send, one_own, one_recv, two_send, two_own,
           two_recv, final, sem_a, sem_g, sem_hs, sem_hr, sem_1s, sem_1r, sem_2s, sem_2r, sem_fin, sem_3s, sem_3r,
           sem_4s, sem_4r, sem_5s, sem_5r, sem_6s, sem_6r, sem_7s, sem_7r):
    mats, tokens, d, ff = dims
    row_blocks, col_blocks = d // ROWS, ff // COLS
    steps = mats * row_blocks * col_blocks
    half, quarter, eighth = ROWS // 2, ROWS // 4, ROWS // 8
    after = steps - AFTER

    me = lax.axis_index("dp")
    core, first_bit, second_bit = position(me)
    mate = me + 1 - 2 * core
    first = me + (1 - 2 * first_bit) * (4 - 2 * core)
    second = me + (1 - 2 * second_bit) * (2 + 2 * core)

    def send(src, dst, send_sem, recv_sem, to):
        return pltpu.make_async_remote_copy(src, dst, send_sem, recv_sem, device_id={"dp": to}, device_id_type=MESH)

    barrier = pltpu.get_barrier_semaphore()
    for to in (mate, first, second):
        pl.semaphore_signal(barrier, 1, device_id={"dp": to}, device_id_type=MESH)

    def load_a(n, r):
        cols = pl.ds(pl.multiple_of(r * ROWS, ROWS), ROWS)
        return pltpu.make_async_copy(a.at[0, n, :, cols], a_v.at[n % 2, :, cols], sem_a.at[n % 2, r])

    def load_g(i):
        n, c = i // col_blocks, i % col_blocks
        cols = pl.ds(pl.multiple_of(c * COLS, 128), COLS)
        return pltpu.make_async_copy(g.at[0, n, :, cols], g_v.at[i % 2], sem_g.at[i % 2])

    def rows_of(k, start, size):
        return out.at[index(dims, k, start, size)]

    own_half = core * half
    here = own_half + first_bit * quarter + second_bit * eighth
    there = own_half + first_bit * quarter + (1 - second_bit) * eighth
    across = own_half + (1 - first_bit) * quarter + second_bit * eighth

    def swap(k):
        return send(half_send.at[k % 2], half_recv.at[k % 2], sem_hs.at[k % 2], sem_hr.at[k % 2], mate)

    def exchange_one(k):
        return send(one_send.at[k % RING_ONE], one_recv.at[k % RING_ONE], sem_1s.at[k % RING_ONE], sem_1r.at[k % RING_ONE], first)

    def exchange_two(k):
        return send(two_send.at[k % RING_TWO], two_recv.at[k % RING_TWO], sem_2s.at[k % RING_TWO], sem_2r.at[k % RING_TWO], second)

    def keep(k):
        return pltpu.make_async_copy(final.at[k], rows_of(k, here, eighth), sem_fin.at[k])

    def gather_second(k):
        return send(final.at[k], rows_of(k, here, eighth), sem_3s.at[k], sem_3r.at[k], second)

    def gather_later(k):
        return send(final.at[k], later.at[k - after], sem_3s.at[k], sem_3r.at[k], second)

    def gather_first(k):
        return send(final.at[k], rows_of(k, here, eighth), sem_4s.at[k], sem_4r.at[k], first)

    def relay(k):
        return send(rows_of(k, there, eighth), rows_of(k, there, eighth), sem_5s.at[k], sem_5r.at[k], first)

    def hand_over(k):
        return send(rows_of(k, own_half, half), rows_of(k, own_half, half), sem_6s.at[k], sem_6r.at[k], mate)

    def hand_over_own(k):
        return send(final.at[k], rows_of(k, here, eighth), sem_6s.at[k], sem_6r.at[k], mate)

    def hand_over_later(k):
        return send(later.at[k - after], rows_of(k, there, eighth), sem_5s.at[k], sem_5r.at[k], mate)

    def hand_over_across(k):
        return send(rows_of(k, across, eighth), rows_of(k, across, eighth), sem_7s.at[k - after], sem_7r.at[k - after], mate)

    def product(k, start):
        n, c, r = place(dims, k)
        cols = pl.ds(pl.multiple_of(r * ROWS + start, half), half)
        return lax.dot_general(
            a_v[n % 2, :, cols], g_v[(k // row_blocks) % 2], (((0,), (0,)), ((), ())), preferred_element_type=jnp.float32
        )

    def part(ref, slot, bit, size):
        return ref[slot, pl.ds(pl.multiple_of(bit * size, size), size), :]

    def reduce_cores(k):
        swap(k).wait_recv()

        @pl.when(k >= RING_ONE)
        def _():
            exchange_one(k - RING_ONE).wait_send()

        def total(bit):
            return part(half_own, k % 2, bit, quarter) + part(half_recv, k % 2, bit, quarter).astype(jnp.float32)

        one_send[k % RING_ONE] = total(1 - first_bit).astype(jnp.bfloat16)
        one_own[k % OWN_ONE] = total(first_bit)
        exchange_one(k).start()

    def reduce_first(k):
        exchange_one(k).wait_recv()

        @pl.when(k >= RING_TWO)
        def _():
            exchange_two(k - RING_TWO).wait_send()

        def total(bit):
            return part(one_own, k % OWN_ONE, bit, eighth) + part(one_recv, k % RING_ONE, bit, eighth).astype(jnp.float32)

        two_send[k % RING_TWO] = total(1 - second_bit).astype(jnp.bfloat16)
        two_own[k % OWN_TWO] = total(second_bit)
        exchange_two(k).start()

    def reduce_second(k):
        exchange_two(k).wait_recv()
        final[k] = (two_own[k % OWN_TWO] + two_recv[k % RING_TWO].astype(jnp.float32)).astype(jnp.bfloat16)
        keep(k).start()

    def either(k, before, tail):
        pl.when(k < after)(before)
        pl.when(k >= after)(tail)

    def gather(k):
        def before():
            gather_second(k).start()

        def tail():
            gather_later(k).start()
            hand_over_own(k).start()

        either(k, before, tail)
        gather_first(k).start()

    def pass_on(k):
        def before():
            gather_second(k).wait_recv()
            relay(k).start()

        def tail():
            gather_later(k).wait_recv()
            hand_over_later(k).start()

        either(k, before, tail)

    def finish(k):
        keep(k).wait()
        gather_first(k).wait_recv()

        def before():
            relay(k).wait_recv()
            hand_over(k).start()

        def tail():
            hand_over_across(k).start()

        either(k, before, tail)

    load_a(0, 0).start()
    load_g(0).start()
    for r in range(1, row_blocks):
        load_a(0, r).start()
    pl.semaphore_wait(barrier, 3)

    def step(k, carry):
        n, c, r = place(dims, k)

        @pl.when(r == 0)
        def _():
            load_g(k // row_blocks).wait()

            @pl.when(k + row_blocks < steps)
            def _():
                load_g(k // row_blocks + 1).start()

        @pl.when(c == 0)
        def _():
            load_a(n, r).wait()

            @pl.when(n + 1 < mats)
            def _():
                load_a(n + 1, r).start()

        @pl.when(k >= 2)
        def _():
            swap(k - 2).wait_send()

        half_send[k % 2] = product(k, (1 - core) * half).astype(jnp.bfloat16)
        swap(k).start()
        half_own[k % 2] = product(k, own_half)
        reduce_cores(k)

        @pl.when(k >= LAG_ONE)
        def _():
            reduce_first(k - LAG_ONE)

        @pl.when(k >= LAG_TWO)
        def _():
            reduce_second(k - LAG_TWO)

        since = k - GATHER_FROM

        @pl.when((since >= 0) & (since % GATHER_SKIP != GATHER_SKIP - 1))
        def _():
            i = since - since // GATHER_SKIP
            gather(i)

            @pl.when(i >= PASS_LAG)
            def _():
                pass_on(i - PASS_LAG)

            @pl.when(i >= FINISH_LAG)
            def _():
                finish(i - FINISH_LAG)

        return carry

    lax.fori_loop(0, steps, step, 0)
    since = steps - GATHER_FROM
    started = since - since // GATHER_SKIP

    def loop(low, high, f):
        def body(k, carry):
            f(k)
            return carry

        lax.fori_loop(low, high, body, 0)

    for k in range(steps, steps + LAG_TWO):
        if k - LAG_ONE < steps:
            reduce_first(k - LAG_ONE)
        reduce_second(k - LAG_TWO)
        ready = min(started + TAIL, k - LAG_TWO + 1) if k + 1 < steps + LAG_TWO else steps
        loop(started, ready, gather)
        started = max(started, ready)
    loop(since - since // GATHER_SKIP - PASS_LAG, steps, pass_on)
    loop(since - since // GATHER_SKIP - FINISH_LAG, steps, finish)

    def drain(k):
        gather_first(k).wait_send()

        def before():
            gather_second(k).wait_send()
            relay(k).wait_send()
            hand_over(k).wait()

        def tail():
            gather_later(k).wait_send()
            hand_over_own(k).wait()
            hand_over_later(k).wait()
            hand_over_across(k).wait()

        either(k, before, tail)

    loop(0, steps, drain)
    for k in range(steps - 2, steps):
        swap(k).wait_send()
    for k in range(steps - RING_ONE, steps):
        exchange_one(k).wait_send()
    for k in range(steps - RING_TWO, steps):
        exchange_two(k).wait_send()


def copy_kernel(mats, d, src, dst, buffer, sem_in, sem_out):
    blocks = [(n, r) for n in range(mats) for r in range(0, d, COPY_ROWS)]

    def load(i):
        n, r = blocks[i]
        return pltpu.make_async_copy(src.at[n, pl.ds(r, COPY_ROWS)], buffer.at[i % COPY_SLOTS], sem_in.at[i % COPY_SLOTS])

    def store(i):
        n, r = blocks[i]
        return pltpu.make_async_copy(buffer.at[i % COPY_SLOTS], dst.at[n, pl.ds(r, COPY_ROWS)], sem_out.at[i % COPY_SLOTS])

    ahead = COPY_SLOTS // 2
    for i in range(ahead):
        load(i).start()
    for i in range(len(blocks)):
        load(i).wait()
        store(i).start()
        if i + ahead < len(blocks):
            if i + ahead >= COPY_SLOTS:
                store(i + ahead - COPY_SLOTS).wait()
            load(i + ahead).start()
    for i in range(len(blocks) - COPY_SLOTS, len(blocks)):
        store(i).wait()


def put_kernel(dims, starts, steps, *refs):
    count = len(starts)
    sources, dst, buffer, sem_in, sem_out = refs[:count], refs[count + 1], refs[-3], refs[-2], refs[-1]
    eighth = ROWS // 8
    rows = [start(lax.axis_index("dp")) for start in starts]

    def load(i):
        return pltpu.make_async_copy(sources[i], buffer.at[i], sem_in.at[i])

    def store(i, j):
        place = dst.at[index(dims, steps - AFTER + j, rows[i], eighth)]
        return pltpu.make_async_copy(buffer.at[i, j], place, sem_out.at[i, j])

    for i in range(count):
        load(i).start()
    for i in range(count):
        load(i).wait()
        for j in range(AFTER):
            store(i, j).start()
    for i in range(count):
        for j in range(AFTER):
            store(i, j).wait()


def there_of(me):
    core, first_bit, second_bit = position(me)
    return core * (ROWS // 2) + first_bit * (ROWS // 4) + (1 - second_bit) * (ROWS // 8)


def opposite_of(me):
    core, first_bit, second_bit = position(me)
    return core * (ROWS // 2) + (1 - first_bit) * (ROWS // 4) + (1 - second_bit) * (ROWS // 8)


def mates_opposite_of(me):
    core, first_bit, second_bit = position(me)
    return (1 - core) * (ROWS // 2) + (1 - second_bit) * (ROWS // 4) + (1 - first_bit) * (ROWS // 8)


def solution(mesh):
    def step(a, g):
        _, mats, tokens, d = a.shape
        ff = g.shape[-1]
        steps = mats * (d // ROWS) * (ff // COLS)
        half, quarter, eighth = ROWS // 2, ROWS // 4, ROWS // 8
        bf16, f32 = jnp.bfloat16, jnp.float32
        dma = pltpu.SemaphoreType.DMA
        dims = (mats, tokens, d, ff)
        whole = jax.ShapeDtypeStruct((mats, d, ff), bf16)
        hbm = pl.BlockSpec(memory_space=pl.ANY)
        summed, later = pl.pallas_call(
            functools.partial(kernel, dims),
            out_shape=(whole, jax.ShapeDtypeStruct((AFTER, eighth, COLS), bf16)),
            in_specs=[pl.BlockSpec(memory_space=pl.ANY)] * 2,
            out_specs=(hbm, hbm),
            scratch_shapes=[
                pltpu.VMEM((2, tokens, d), bf16),
                pltpu.VMEM((2, tokens, COLS), bf16),
                pltpu.VMEM((2, half, COLS), bf16),
                pltpu.VMEM((2, half, COLS), f32),
                pltpu.VMEM((2, half, COLS), bf16),
                pltpu.VMEM((RING_ONE, quarter, COLS), bf16),
                pltpu.VMEM((OWN_ONE, quarter, COLS), f32),
                pltpu.VMEM((RING_ONE, quarter, COLS), bf16),
                pltpu.VMEM((RING_TWO, eighth, COLS), bf16),
                pltpu.VMEM((OWN_TWO, eighth, COLS), f32),
                pltpu.VMEM((RING_TWO, eighth, COLS), bf16),
                pltpu.VMEM((steps, eighth, COLS), bf16),
                dma((2, d // ROWS)),
                dma((2,)),
                dma((2,)),
                dma((2,)),
                dma((RING_ONE,)),
                dma((RING_ONE,)),
                dma((RING_TWO,)),
                dma((RING_TWO,)),
            ]
            + [dma((steps,))] * 9
            + [dma((AFTER,))] * 2,
            compiler_params=pltpu.CompilerParams(
                collective_id=0, has_side_effects=True, vmem_limit_bytes=VMEM_LIMIT
            ),
        )(a, g)

        opposite = lax.ppermute(later, "dp", [(i, i ^ (2 if i % 2 else 4)) for i in range(8)])
        result = pl.pallas_call(
            functools.partial(copy_kernel, mats, d),
            out_shape=whole,
            in_specs=[hbm],
            out_specs=hbm,
            scratch_shapes=[pltpu.VMEM((COPY_SLOTS, COPY_ROWS, ff), bf16), dma((COPY_SLOTS,)), dma((COPY_SLOTS,))],
            compiler_params=pltpu.CompilerParams(vmem_limit_bytes=50 * 2**20),
            cost_estimate=pl.CostEstimate(flops=2 * 10**9, bytes_accessed=4 * mats * d * ff, transcendentals=0),
            name="copy",
        )(summed)

        def put(result, *sources_and_starts):
            sources, starts = sources_and_starts[::2], sources_and_starts[1::2]
            return pl.pallas_call(
                functools.partial(put_kernel, dims, starts, steps),
                out_shape=whole,
                in_specs=[hbm] * (len(sources) + 1),
                out_specs=hbm,
                scratch_shapes=[
                    pltpu.VMEM((len(sources), AFTER, eighth, COLS), bf16),
                    dma((len(sources),)),
                    dma((len(sources), AFTER)),
                ],
                input_output_aliases={len(sources): 0},
                compiler_params=pltpu.CompilerParams(vmem_limit_bytes=16 * 2**20),
                cost_estimate=pl.CostEstimate(flops=2 * 10**8, bytes_accessed=4 * len(sources) * later.size, transcendentals=0),
                name="put",
            )(*sources, result)

        opposite, result = lax.optimization_barrier((opposite, result))
        mates = lax.ppermute(opposite, "dp", [(i, i ^ 1) for i in range(8)])
        result = put(result, later, there_of, opposite, opposite_of)
        return put(result, mates, mates_opposite_of)

    return jax.shard_map(
        step,
        mesh=mesh,
        in_specs=(P(("rep", "dp")), P(("rep", "dp"))),
        out_specs=P("rep"),
        check_vma=False,
    )
```

```python
import functools

import jax
import jax.numpy as jnp
from jax import lax
from jax.experimental import pallas as pl
from jax.experimental.pallas import tpu as pltpu
from jax.sharding import PartitionSpec as P

MESH = pl.DeviceIdType.MESH
ROWS, COLS = 512, 640
VMEM_LIMIT = 63 * 2**20
LAG_ONE, LAG_TWO = 2, 4
RING_ONE, RING_TWO = 2 * LAG_ONE + 2, 2 * (LAG_TWO - LAG_ONE) + 2
OWN_ONE, OWN_TWO = LAG_ONE + 1, LAG_TWO - LAG_ONE + 1
SHORT_UNTIL = 5
GATHER_SKIP = 8
PIECES = 4
PASS_LAG, FINISH_LAG, DRAIN_LAG = 2, 4, 8
COPY_SLOTS = 16

TAIL = 2


def position(me):
    core, y, x = me % 2, (me // 2) % 2, me // 4
    return core, x * (1 - core) + y * core, y * (1 - core) + x * core


def place(dims, k):
    mats, tokens, d, ff = dims
    row_blocks, col_blocks = d // ROWS, ff // COLS
    rest = k % (row_blocks * col_blocks)
    return k // (row_blocks * col_blocks), rest // row_blocks, rest % row_blocks


def index(dims, k, start, size):
    n, c, r = place(dims, k)
    return n, pl.ds(pl.multiple_of(r * ROWS + start, size), size), pl.ds(pl.multiple_of(c * COLS, 128), COLS)


def kernel(dims, a, g, out, later, a_v, g_v, half_send, half_own, half_recv, one_send, one_own, one_recv, two_send, two_own,
           two_recv, final, sem_a, sem_g, sem_hs, sem_hr, sem_1s, sem_1r, sem_2s, sem_2r, sem_fin, sem_3s, sem_3r,
           sem_4s, sem_4r, sem_5s, sem_5r, sem_6s, sem_6r, sem_7s, sem_7r,
           sem_first):
    mats, tokens, d, ff = dims
    row_blocks, col_blocks = d // ROWS, ff // COLS
    steps = mats * row_blocks * col_blocks
    half, quarter, eighth = ROWS // 2, ROWS // 4, ROWS // 8

    me = lax.axis_index("dp")
    core, first_bit, second_bit = position(me)
    mate = me + 1 - 2 * core
    first = me + (1 - 2 * first_bit) * (4 - 2 * core)
    second = me + (1 - 2 * second_bit) * (2 + 2 * core)

    def send(src, dst, send_sem, recv_sem, to):
        return pltpu.make_async_remote_copy(src, dst, send_sem, recv_sem, device_id={"dp": to}, device_id_type=MESH)

    barrier = pltpu.get_barrier_semaphore()
    for to in (mate, first, second):
        pl.semaphore_signal(barrier, 1, device_id={"dp": to}, device_id_type=MESH)

    def load_a(n, r):
        cols = pl.ds(pl.multiple_of(r * ROWS, ROWS), ROWS)
        return pltpu.make_async_copy(a.at[0, n, :, cols], a_v.at[n % 2, :, cols], sem_a.at[n % 2, r])

    def load_g(i):
        n, c = i // col_blocks, i % col_blocks
        cols = pl.ds(pl.multiple_of(c * COLS, 128), COLS)
        return pltpu.make_async_copy(g.at[0, n, :, cols], g_v.at[i % 2], sem_g.at[i % 2])

    def load_first(i):
        size = tokens // PIECES
        piece = pl.ds(i * size, size)
        return (
            pltpu.make_async_copy(a.at[0, 0, piece, pl.ds(0, ROWS)], a_v.at[0, piece, pl.ds(0, ROWS)], sem_first.at[0, i]),
            pltpu.make_async_copy(g.at[0, 0, piece, pl.ds(0, COLS)], g_v.at[0, piece], sem_first.at[1, i]),
        )

    def rows_of(k, start, size):
        return out.at[k, pl.ds(pl.multiple_of(start, eighth), size)]

    own_half = core * half
    here = own_half + first_bit * quarter + second_bit * eighth
    there = own_half + first_bit * quarter + (1 - second_bit) * eighth
    across = own_half + (1 - first_bit) * quarter + second_bit * eighth

    def swap(k):
        return send(half_send.at[k % 2], half_recv.at[k % 2], sem_hs.at[k % 2], sem_hr.at[k % 2], mate)

    def exchange_one(k):
        return send(one_send.at[k % RING_ONE], one_recv.at[k % RING_ONE], sem_1s.at[k % RING_ONE], sem_1r.at[k % RING_ONE], first)

    def exchange_two(k):
        return send(two_send.at[k % RING_TWO], two_recv.at[k % RING_TWO], sem_2s.at[k % RING_TWO], sem_2r.at[k % RING_TWO], second)

    def keep(k):
        return pltpu.make_async_copy(final.at[k], rows_of(k, here, eighth), sem_fin.at[k])

    def gather_second(k):
        return send(final.at[k], rows_of(k, here, eighth), sem_3s.at[k], sem_3r.at[k], second)

    def gather_later(k):
        return send(final.at[k], later.at[k // 2], sem_3s.at[k], sem_3r.at[k], second)

    def gather_first(k):
        return send(final.at[k], rows_of(k, here, eighth), sem_4s.at[k], sem_4r.at[k], first)

    def relay(k):
        return send(rows_of(k, there, eighth), rows_of(k, there, eighth), sem_5s.at[k], sem_5r.at[k], first)

    def hand_over(k):
        return send(rows_of(k, own_half, half), rows_of(k, own_half, half), sem_6s.at[k], sem_6r.at[k], mate)

    def hand_over_own(k):
        return send(final.at[k], rows_of(k, here, eighth), sem_6s.at[k], sem_6r.at[k], mate)

    def hand_over_later(k):
        return send(later.at[k // 2], rows_of(k, there, eighth), sem_5s.at[k], sem_5r.at[k], mate)

    def hand_over_across(k):
        return send(rows_of(k, across, eighth), rows_of(k, across, eighth), sem_7s.at[k // 2], sem_7r.at[k // 2], mate)

    def product(k, start):
        n, c, r = place(dims, k)
        cols = pl.ds(pl.multiple_of(r * ROWS + start, half), half)
        return lax.dot_general(
            a_v[n % 2, :, cols], g_v[(k // row_blocks) % 2], (((0,), (0,)), ((), ())), preferred_element_type=jnp.float32
        )

    def part(ref, slot, bit, size):
        return ref[slot, pl.ds(pl.multiple_of(bit * size, size), size), :]

    def reduce_cores(k):
        swap(k).wait_recv()

        @pl.when(k >= RING_ONE)
        def _():
            exchange_one(k - RING_ONE).wait_send()

        def total(bit):
            return part(half_own, k % 2, bit, quarter) + part(half_recv, k % 2, bit, quarter).astype(jnp.float32)

        one_send[k % RING_ONE] = total(1 - first_bit).astype(jnp.bfloat16)
        one_own[k % OWN_ONE] = total(first_bit)
        exchange_one(k).start()

    def reduce_first(k):
        exchange_one(k).wait_recv()

        @pl.when(k >= RING_TWO)
        def _():
            exchange_two(k - RING_TWO).wait_send()

        def total(bit):
            return part(one_own, k % OWN_ONE, bit, eighth) + part(one_recv, k % RING_ONE, bit, eighth).astype(jnp.float32)

        two_send[k % RING_TWO] = total(1 - second_bit).astype(jnp.bfloat16)
        two_own[k % OWN_TWO] = total(second_bit)
        exchange_two(k).start()

    def reduce_second(k):
        exchange_two(k).wait_recv()
        final[k] = (two_own[k % OWN_TWO] + two_recv[k % RING_TWO].astype(jnp.float32)).astype(jnp.bfloat16)
        keep(k).start()

    def either(k, before, tail):
        pl.when(k % 2 == 0)(before)
        pl.when(k % 2 == 1)(tail)

    def gather(k):
        def before():
            gather_second(k).start()

        def tail():
            gather_later(k).start()
            hand_over_own(k).start()

        either(k, before, tail)
        gather_first(k).start()

    def pass_on(k):
        def before():
            gather_second(k).wait_recv()
            relay(k).start()

        def tail():
            gather_later(k).wait_recv()
            hand_over_later(k).start()

        either(k, before, tail)

    def finish(k):
        keep(k).wait()
        gather_first(k).wait_recv()

        def before():
            relay(k).wait_recv()
            hand_over(k).start()

        def tail():
            hand_over_across(k).start()

        either(k, before, tail)

    def drain(k):
        gather_first(k).wait_send()

        def before():
            gather_second(k).wait_send()
            relay(k).wait_send()
            hand_over(k).wait()

        def tail():
            gather_later(k).wait_send()
            hand_over_own(k).wait()
            hand_over_later(k).wait()
            hand_over_across(k).wait()

        either(k, before, tail)

    for i in range(PIECES):
        for copy in load_first(i):
            copy.start()
    mates_cols = pl.ds(pl.multiple_of((1 - core) * half, half), half)
    for i in range(PIECES):
        for copy in load_first(i):
            copy.wait()
        if i == PIECES - 1:
            for r in range(1, row_blocks):
                load_a(0, r).start()
        piece = pl.ds(i * (tokens // PIECES), tokens // PIECES)
        one = lax.dot_general(
            a_v[0, piece, mates_cols], g_v[0, piece], (((0,), (0,)), ((), ())), preferred_element_type=jnp.float32
        )
        if i == 0:
            half_own[0] = one
        elif i < PIECES - 1:
            half_own[0] += one
        else:
            half_send[0] = (half_own[0] + one).astype(jnp.bfloat16)
    pl.semaphore_wait(barrier, 3)

    def step(k, carry):
        n, c, r = place(dims, k)

        @pl.when(r == 0)
        def _():
            @pl.when(k > 0)
            def _():
                load_g(k // row_blocks).wait()

            @pl.when(k + row_blocks < steps)
            def _():
                load_g(k // row_blocks + 1).start()

        @pl.when(c == 0)
        def _():
            @pl.when(k > 0)
            def _():
                load_a(n, r).wait()

            @pl.when(n + 1 < mats)
            def _():
                load_a(n + 1, r).start()

        @pl.when(k >= 2)
        def _():
            swap(k - 2).wait_send()

        @pl.when(k > 0)
        def _():
            half_send[k % 2] = product(k, (1 - core) * half).astype(jnp.bfloat16)

        swap(k).start()
        half_own[k % 2] = product(k, own_half)
        reduce_cores(k)

        more = jnp.minimum(k // SHORT_UNTIL, 1)

        @pl.when((k >= 1) & (k != SHORT_UNTIL))
        def _():
            reduce_first(k - 1 - (LAG_ONE - 1) * more)

        @pl.when((k >= 2) & (k != SHORT_UNTIL) & (k != SHORT_UNTIL + 1))
        def _():
            reduce_second(k - 2 - (LAG_TWO - 2) * more)

        since = k - SHORT_UNTIL - LAG_TWO + 2
        skipped = more * (LAG_TWO - 2 + since // GATHER_SKIP)
        now = (k < SHORT_UNTIL) | ((since >= 0) & (since % GATHER_SKIP != GATHER_SKIP - 1))

        @pl.when((k >= 2) & now)
        def _():
            i = k - 2 - skipped
            gather(i)

            @pl.when(i >= PASS_LAG)
            def _():
                pass_on(i - PASS_LAG)

            @pl.when(i >= FINISH_LAG)
            def _():
                finish(i - FINISH_LAG)

            @pl.when(i >= DRAIN_LAG)
            def _():
                drain(i - DRAIN_LAG)

        return carry

    lax.fori_loop(0, steps, step, 0)
    started = steps - LAG_TWO - (steps - SHORT_UNTIL - LAG_TWO + 2) // GATHER_SKIP
    passed, finished, drained = started - PASS_LAG, started - FINISH_LAG, started - DRAIN_LAG

    def loop(low, high, f):
        def body(k, carry):
            f(k)
            return carry

        lax.fori_loop(low, high, body, 0)

    for k in range(steps, steps + LAG_TWO):
        if k - LAG_ONE < steps:
            reduce_first(k - LAG_ONE)
        reduce_second(k - LAG_TWO)
        ready = min(started + TAIL, k - LAG_TWO + 1) if k + 1 < steps + LAG_TWO else steps
        loop(started, ready, gather)
        started = max(started, ready)
    loop(passed, steps, pass_on)

    def finish_and_drain(k):
        finish(k)
        drain(k - DRAIN_LAG + FINISH_LAG)

    loop(finished, steps, finish_and_drain)
    loop(steps - DRAIN_LAG + FINISH_LAG, steps, drain)
    for k in range(steps - 2, steps):
        swap(k).wait_send()
    for k in range(steps - RING_ONE, steps):
        exchange_one(k).wait_send()
    for k in range(steps - RING_TWO, steps):
        exchange_two(k).wait_send()


def copy_kernel(dims, src, dst, buffer, sem_in, sem_out):
    steps = src.shape[0]

    def load(i):
        return pltpu.make_async_copy(src.at[i], buffer.at[i % COPY_SLOTS], sem_in.at[i % COPY_SLOTS])

    def store(i):
        return pltpu.make_async_copy(
            buffer.at[i % COPY_SLOTS], dst.at[index(dims, i, 0, ROWS)], sem_out.at[i % COPY_SLOTS]
        )

    ahead = COPY_SLOTS // 2
    for i in range(ahead):
        load(i).start()
    for i in range(steps):
        load(i).wait()
        store(i).start()
        if i + ahead < steps:
            if i + ahead >= COPY_SLOTS:
                store(i + ahead - COPY_SLOTS).wait()
            load(i + ahead).start()
    for i in range(steps - COPY_SLOTS, steps):
        store(i).wait()


def put_kernel(dims, starts, *refs):
    count = len(starts)
    sources, dst, sem = refs[:count], refs[count + 1], refs[-1]
    rows = [start(lax.axis_index("dp")) for start in starts]

    def store(i, j):
        return pltpu.make_async_copy(sources[i].at[j], dst.at[index(dims, 2 * j + 1, rows[i], ROWS // 8)], sem.at[i, j])

    for i in range(count):
        for j in range(sources[i].shape[0]):
            store(i, j).start()
    for i in range(count):
        for j in range(sources[i].shape[0]):
            store(i, j).wait()


def there_of(me):
    core, first_bit, second_bit = position(me)
    return core * (ROWS // 2) + first_bit * (ROWS // 4) + (1 - second_bit) * (ROWS // 8)


def opposite_of(me):
    core, first_bit, second_bit = position(me)
    return core * (ROWS // 2) + (1 - first_bit) * (ROWS // 4) + (1 - second_bit) * (ROWS // 8)


def mates_opposite_of(me):
    core, first_bit, second_bit = position(me)
    return (1 - core) * (ROWS // 2) + (1 - second_bit) * (ROWS // 4) + (1 - first_bit) * (ROWS // 8)


def solution(mesh):
    def step(a, g):
        _, mats, tokens, d = a.shape
        ff = g.shape[-1]
        steps = mats * (d // ROWS) * (ff // COLS)
        half, quarter, eighth = ROWS // 2, ROWS // 4, ROWS // 8
        bf16, f32 = jnp.bfloat16, jnp.float32
        dma = pltpu.SemaphoreType.DMA
        dims = (mats, tokens, d, ff)
        whole = jax.ShapeDtypeStruct((mats, d, ff), bf16)
        hbm = pl.BlockSpec(memory_space=pl.ANY)
        summed, later = pl.pallas_call(
            functools.partial(kernel, dims),
            out_shape=(jax.ShapeDtypeStruct((steps, ROWS, COLS), bf16), jax.ShapeDtypeStruct((steps // 2, eighth, COLS), bf16)),
            in_specs=[pl.BlockSpec(memory_space=pl.ANY)] * 2,
            out_specs=(hbm, hbm),
            scratch_shapes=[
                pltpu.VMEM((2, tokens, d), bf16),
                pltpu.VMEM((2, tokens, COLS), bf16),
                pltpu.VMEM((2, half, COLS), bf16),
                pltpu.VMEM((2, half, COLS), f32),
                pltpu.VMEM((2, half, COLS), bf16),
                pltpu.VMEM((RING_ONE, quarter, COLS), bf16),
                pltpu.VMEM((OWN_ONE, quarter, COLS), f32),
                pltpu.VMEM((RING_ONE, quarter, COLS), bf16),
                pltpu.VMEM((RING_TWO, eighth, COLS), bf16),
                pltpu.VMEM((OWN_TWO, eighth, COLS), f32),
                pltpu.VMEM((RING_TWO, eighth, COLS), bf16),
                pltpu.VMEM((steps, eighth, COLS), bf16),
                dma((2, d // ROWS)),
                dma((2,)),
                dma((2,)),
                dma((2,)),
                dma((RING_ONE,)),
                dma((RING_ONE,)),
                dma((RING_TWO,)),
                dma((RING_TWO,)),
            ]
            + [dma((steps,))] * 9
            + [dma((steps // 2,))] * 2
            + [dma((2, PIECES))],
            compiler_params=pltpu.CompilerParams(
                collective_id=0, has_side_effects=True, vmem_limit_bytes=VMEM_LIMIT
            ),
        )(a, g)

        opposite = lax.ppermute(later, "dp", [(i, i ^ (2 if i % 2 else 4)) for i in range(8)])
        result = pl.pallas_call(
            functools.partial(copy_kernel, dims),
            out_shape=whole,
            in_specs=[hbm],
            out_specs=hbm,
            scratch_shapes=[pltpu.VMEM((COPY_SLOTS, ROWS, COLS), bf16), dma((COPY_SLOTS,)), dma((COPY_SLOTS,))],
            compiler_params=pltpu.CompilerParams(vmem_limit_bytes=50 * 2**20),
            cost_estimate=pl.CostEstimate(flops=2 * 10**9, bytes_accessed=4 * mats * d * ff, transcendentals=0),
            name="copy",
        )(summed)

        def put(result, *sources_and_starts):
            sources, starts = sources_and_starts[::2], sources_and_starts[1::2]
            return pl.pallas_call(
                functools.partial(put_kernel, dims, starts),
                out_shape=whole,
                in_specs=[hbm] * (len(sources) + 1),
                out_specs=hbm,
                scratch_shapes=[dma((len(sources), steps // 2))],
                input_output_aliases={len(sources): 0},
                compiler_params=pltpu.CompilerParams(vmem_limit_bytes=16 * 2**20),
                cost_estimate=pl.CostEstimate(flops=2 * 10**8, bytes_accessed=4 * len(sources) * later.size, transcendentals=0),
                name="put",
            )(*sources, result)

        opposite, result = lax.optimization_barrier((opposite, result))
        mates = lax.ppermute(opposite, "dp", [(i, i ^ 1) for i in range(8)])
        result = put(result, later, there_of, opposite, opposite_of)
        return put(result, mates, mates_opposite_of)

    return jax.shard_map(
        step,
        mesh=mesh,
        in_specs=(P(("rep", "dp")), P(("rep", "dp"))),
        out_specs=P("rep"),
        check_vma=False,
    )
```

```python
import functools

import jax
import jax.numpy as jnp
from jax import lax
from jax.experimental import pallas as pl
from jax.experimental.pallas import tpu as pltpu
from jax.sharding import PartitionSpec as P

MESH = pl.DeviceIdType.MESH
ROWS, COLS = 512, 640
VMEM_LIMIT = 63 * 2**20
LAG_ONE, LAG_TWO = 2, 4
RING_ONE, RING_TWO = 2 * LAG_ONE + 2, 2 * (LAG_TWO - LAG_ONE) + 2
OWN_ONE, OWN_TWO = LAG_ONE + 1, LAG_TWO - LAG_ONE + 1
SHORT_UNTIL = 5
GATHER_SKIP = 8
PIECES = 4
PASS_LAG, FINISH_LAG, DRAIN_LAG = 2, 4, 8
COPY_SLOTS = 16

TAIL = 2


def position(me):
    core, y, x = me % 2, (me // 2) % 2, me // 4
    return core, x * (1 - core) + y * core, y * (1 - core) + x * core


def place(dims, k):
    mats, tokens, d, ff = dims
    row_blocks, col_blocks = d // ROWS, ff // COLS
    rest = k % (row_blocks * col_blocks)
    return k // (row_blocks * col_blocks), rest // row_blocks, rest % row_blocks


def index(dims, k, start, size):
    n, c, r = place(dims, k)
    return n, pl.ds(pl.multiple_of(r * ROWS + start, size), size), pl.ds(pl.multiple_of(c * COLS, 128), COLS)


def kernel(dims, a, g, out, later, a_v, g_v, half_send, half_own, half_recv, one_send, one_own, one_recv, two_send, two_own,
           two_recv, final, sem_a, sem_g, sem_hs, sem_hr, sem_1s, sem_1r, sem_2s, sem_2r, sem_fin, sem_3s, sem_3r,
           sem_4s, sem_4r, sem_5s, sem_5r, sem_6s, sem_6r, sem_7s, sem_7r,
           sem_first):
    mats, tokens, d, ff = dims
    row_blocks, col_blocks = d // ROWS, ff // COLS
    steps = mats * row_blocks * col_blocks
    half, quarter, eighth = ROWS // 2, ROWS // 4, ROWS // 8

    me = lax.axis_index("dp")
    core, first_bit, second_bit = position(me)
    mate = me + 1 - 2 * core
    first = me + (1 - 2 * first_bit) * (4 - 2 * core)
    second = me + (1 - 2 * second_bit) * (2 + 2 * core)

    def send(src, dst, send_sem, recv_sem, to):
        return pltpu.make_async_remote_copy(src, dst, send_sem, recv_sem, device_id={"dp": to}, device_id_type=MESH)

    barrier = pltpu.get_barrier_semaphore()
    for to in (mate, first, second):
        pl.semaphore_signal(barrier, 1, device_id={"dp": to}, device_id_type=MESH)

    def load_a(n, r):
        cols = pl.ds(pl.multiple_of(r * ROWS, ROWS), ROWS)
        return pltpu.make_async_copy(a.at[0, n, :, cols], a_v.at[n % 2, :, cols], sem_a.at[n % 2, r])

    def load_g(i):
        n, c = i // col_blocks, i % col_blocks
        cols = pl.ds(pl.multiple_of(c * COLS, 128), COLS)
        return pltpu.make_async_copy(g.at[0, n, :, cols], g_v.at[i % 2], sem_g.at[i % 2])

    mates_cols = pl.ds(pl.multiple_of((1 - core) * half, half), half)
    own_cols = pl.ds(pl.multiple_of(core * half, half), half)

    def load_own():
        return pltpu.make_async_copy(a.at[0, 0, :, own_cols], a_v.at[0, :, own_cols], sem_a.at[0, 0])

    def load_first(i):
        size = tokens // PIECES
        piece = pl.ds(i * size, size)
        return (
            pltpu.make_async_copy(a.at[0, 0, piece, mates_cols], a_v.at[0, piece, mates_cols], sem_first.at[0, i]),
            pltpu.make_async_copy(g.at[0, 0, piece, pl.ds(0, COLS)], g_v.at[0, piece], sem_first.at[1, i]),
        )

    def rows_of(k, start, size):
        return out.at[k, pl.ds(pl.multiple_of(start, eighth), size)]

    own_half = core * half
    here = own_half + first_bit * quarter + second_bit * eighth
    there = own_half + first_bit * quarter + (1 - second_bit) * eighth
    across = own_half + (1 - first_bit) * quarter + second_bit * eighth

    def swap(k):
        return send(half_send.at[k % 2], half_recv.at[k % 2], sem_hs.at[k % 2], sem_hr.at[k % 2], mate)

    def exchange_one(k):
        return send(one_send.at[k % RING_ONE], one_recv.at[k % RING_ONE], sem_1s.at[k % RING_ONE], sem_1r.at[k % RING_ONE], first)

    def exchange_two(k):
        return send(two_send.at[k % RING_TWO], two_recv.at[k % RING_TWO], sem_2s.at[k % RING_TWO], sem_2r.at[k % RING_TWO], second)

    def keep(k):
        return pltpu.make_async_copy(final.at[k], rows_of(k, here, eighth), sem_fin.at[k])

    def gather_second(k):
        return send(final.at[k], rows_of(k, here, eighth), sem_3s.at[k], sem_3r.at[k], second)

    def gather_later(k):
        return send(final.at[k], later.at[k // 2], sem_3s.at[k], sem_3r.at[k], second)

    def gather_first(k):
        return send(final.at[k], rows_of(k, here, eighth), sem_4s.at[k], sem_4r.at[k], first)

    def relay(k):
        return send(rows_of(k, there, eighth), rows_of(k, there, eighth), sem_5s.at[k], sem_5r.at[k], first)

    def hand_over(k):
        return send(rows_of(k, own_half, half), rows_of(k, own_half, half), sem_6s.at[k], sem_6r.at[k], mate)

    def hand_over_own(k):
        return send(final.at[k], rows_of(k, here, eighth), sem_6s.at[k], sem_6r.at[k], mate)

    def hand_over_later(k):
        return send(later.at[k // 2], rows_of(k, there, eighth), sem_5s.at[k], sem_5r.at[k], mate)

    def hand_over_across(k):
        return send(rows_of(k, across, eighth), rows_of(k, across, eighth), sem_7s.at[k // 2], sem_7r.at[k // 2], mate)

    def product(k, start):
        n, c, r = place(dims, k)
        cols = pl.ds(pl.multiple_of(r * ROWS + start, half), half)
        return lax.dot_general(
            a_v[n % 2, :, cols], g_v[(k // row_blocks) % 2], (((0,), (0,)), ((), ())), preferred_element_type=jnp.float32
        )

    def part(ref, slot, bit, size):
        return ref[slot, pl.ds(pl.multiple_of(bit * size, size), size), :]

    def reduce_cores(k):
        swap(k).wait_recv()

        @pl.when(k >= RING_ONE)
        def _():
            exchange_one(k - RING_ONE).wait_send()

        def total(bit):
            return part(half_own, k % 2, bit, quarter) + part(half_recv, k % 2, bit, quarter).astype(jnp.float32)

        one_send[k % RING_ONE] = total(1 - first_bit).astype(jnp.bfloat16)
        one_own[k % OWN_ONE] = total(first_bit)
        exchange_one(k).start()

    def reduce_first(k):
        exchange_one(k).wait_recv()

        @pl.when(k >= RING_TWO)
        def _():
            exchange_two(k - RING_TWO).wait_send()

        def total(bit):
            return part(one_own, k % OWN_ONE, bit, eighth) + part(one_recv, k % RING_ONE, bit, eighth).astype(jnp.float32)

        two_send[k % RING_TWO] = total(1 - second_bit).astype(jnp.bfloat16)
        two_own[k % OWN_TWO] = total(second_bit)
        exchange_two(k).start()

    def reduce_second(k):
        exchange_two(k).wait_recv()
        final[k] = (two_own[k % OWN_TWO] + two_recv[k % RING_TWO].astype(jnp.float32)).astype(jnp.bfloat16)
        keep(k).start()

    def either(k, before, tail):
        pl.when(k % 2 == 0)(before)
        pl.when(k % 2 == 1)(tail)

    def gather(k):
        def before():
            gather_second(k).start()

        def tail():
            gather_later(k).start()
            hand_over_own(k).start()

        either(k, before, tail)
        gather_first(k).start()

    def pass_on(k):
        def before():
            gather_second(k).wait_recv()
            relay(k).start()

        def tail():
            gather_later(k).wait_recv()
            hand_over_later(k).start()

        either(k, before, tail)

    def finish(k):
        keep(k).wait()
        gather_first(k).wait_recv()

        def before():
            relay(k).wait_recv()
            hand_over(k).start()

        def tail():
            hand_over_across(k).start()

        either(k, before, tail)

    def drain(k):
        gather_first(k).wait_send()

        def before():
            gather_second(k).wait_send()
            relay(k).wait_send()
            hand_over(k).wait()

        def tail():
            gather_later(k).wait_send()
            hand_over_own(k).wait()
            hand_over_later(k).wait()
            hand_over_across(k).wait()

        either(k, before, tail)

    for i in range(PIECES):
        for copy in load_first(i):
            copy.start()
    load_own().start()
    for i in range(PIECES):
        for copy in load_first(i):
            copy.wait()
        if i == PIECES - 1:
            for r in range(1, row_blocks):
                load_a(0, r).start()
        piece = pl.ds(i * (tokens // PIECES), tokens // PIECES)
        one = lax.dot_general(
            a_v[0, piece, mates_cols], g_v[0, piece], (((0,), (0,)), ((), ())), preferred_element_type=jnp.float32
        )
        if i == 0:
            half_own[0] = one
        elif i < PIECES - 1:
            half_own[0] += one
        else:
            half_send[0] = (half_own[0] + one).astype(jnp.bfloat16)
    load_own().wait()
    pl.semaphore_wait(barrier, 3)

    def step(k, carry):
        n, c, r = place(dims, k)

        @pl.when(r == 0)
        def _():
            @pl.when(k > 0)
            def _():
                load_g(k // row_blocks).wait()

            @pl.when(k + row_blocks < steps)
            def _():
                load_g(k // row_blocks + 1).start()

        @pl.when(c == 0)
        def _():
            @pl.when(k > 0)
            def _():
                load_a(n, r).wait()

            @pl.when(n + 1 < mats)
            def _():
                load_a(n + 1, r).start()

        @pl.when(k >= 2)
        def _():
            swap(k - 2).wait_send()

        @pl.when(k > 0)
        def _():
            half_send[k % 2] = product(k, (1 - core) * half).astype(jnp.bfloat16)

        swap(k).start()
        half_own[k % 2] = product(k, own_half)
        reduce_cores(k)

        more = jnp.minimum(k // SHORT_UNTIL, 1)

        @pl.when((k >= 1) & (k != SHORT_UNTIL))
        def _():
            reduce_first(k - 1 - (LAG_ONE - 1) * more)

        @pl.when((k >= 2) & (k != SHORT_UNTIL) & (k != SHORT_UNTIL + 1))
        def _():
            reduce_second(k - 2 - (LAG_TWO - 2) * more)

        since = k - SHORT_UNTIL - LAG_TWO + 2
        skipped = more * (LAG_TWO - 2 + since // GATHER_SKIP)
        now = (k < SHORT_UNTIL) | ((since >= 0) & (since % GATHER_SKIP != GATHER_SKIP - 1))

        @pl.when((k >= 2) & now)
        def _():
            i = k - 2 - skipped
            gather(i)

            @pl.when(i >= PASS_LAG)
            def _():
                pass_on(i - PASS_LAG)

            @pl.when(i >= FINISH_LAG)
            def _():
                finish(i - FINISH_LAG)

            @pl.when(i >= DRAIN_LAG)
            def _():
                drain(i - DRAIN_LAG)

        return carry

    lax.fori_loop(0, steps, step, 0)
    started = steps - LAG_TWO - (steps - SHORT_UNTIL - LAG_TWO + 2) // GATHER_SKIP
    passed, finished, drained = started - PASS_LAG, started - FINISH_LAG, started - DRAIN_LAG

    def loop(low, high, f):
        def body(k, carry):
            f(k)
            return carry

        lax.fori_loop(low, high, body, 0)

    for k in range(steps, steps + LAG_TWO):
        if k - LAG_ONE < steps:
            reduce_first(k - LAG_ONE)
        reduce_second(k - LAG_TWO)
        ready = min(started + TAIL, k - LAG_TWO + 1) if k + 1 < steps + LAG_TWO else steps
        loop(started, ready, gather)
        started = max(started, ready)
    def finish_and_drain(k):
        finish(k)
        drain(k - DRAIN_LAG + FINISH_LAG)

    loop(passed, steps, pass_on)
    loop(finished, steps, finish_and_drain)
    loop(steps - DRAIN_LAG + FINISH_LAG, steps, drain)
    for k in range(steps - 2, steps):
        swap(k).wait_send()
    for k in range(steps - RING_ONE, steps):
        exchange_one(k).wait_send()
    for k in range(steps - RING_TWO, steps):
        exchange_two(k).wait_send()


def copy_kernel(dims, src, dst, buffer, sem_in, sem_out):
    steps = src.shape[0]

    def load(i):
        return pltpu.make_async_copy(src.at[i], buffer.at[i % COPY_SLOTS], sem_in.at[i % COPY_SLOTS])

    def store(i):
        return pltpu.make_async_copy(
            buffer.at[i % COPY_SLOTS], dst.at[index(dims, i, 0, ROWS)], sem_out.at[i % COPY_SLOTS]
        )

    ahead = COPY_SLOTS // 2
    for i in range(ahead):
        load(i).start()
    for i in range(steps):
        load(i).wait()
        store(i).start()
        if i + ahead < steps:
            if i + ahead >= COPY_SLOTS:
                store(i + ahead - COPY_SLOTS).wait()
            load(i + ahead).start()
    for i in range(steps - COPY_SLOTS, steps):
        store(i).wait()


def put_kernel(dims, starts, *refs):
    count = len(starts)
    sources, dst, sem = refs[:count], refs[count + 1], refs[-1]
    rows = [start(lax.axis_index("dp")) for start in starts]

    def store(i, j):
        return pltpu.make_async_copy(sources[i].at[j], dst.at[index(dims, 2 * j + 1, rows[i], ROWS // 8)], sem.at[i, j])

    for i in range(count):
        for j in range(sources[i].shape[0]):
            store(i, j).start()
    for i in range(count):
        for j in range(sources[i].shape[0]):
            store(i, j).wait()


def there_of(me):
    core, first_bit, second_bit = position(me)
    return core * (ROWS // 2) + first_bit * (ROWS // 4) + (1 - second_bit) * (ROWS // 8)


def opposite_of(me):
    core, first_bit, second_bit = position(me)
    return core * (ROWS // 2) + (1 - first_bit) * (ROWS // 4) + (1 - second_bit) * (ROWS // 8)


def mates_opposite_of(me):
    core, first_bit, second_bit = position(me)
    return (1 - core) * (ROWS // 2) + (1 - second_bit) * (ROWS // 4) + (1 - first_bit) * (ROWS // 8)


def solution(mesh):
    def step(a, g):
        _, mats, tokens, d = a.shape
        ff = g.shape[-1]
        steps = mats * (d // ROWS) * (ff // COLS)
        half, quarter, eighth = ROWS // 2, ROWS // 4, ROWS // 8
        bf16, f32 = jnp.bfloat16, jnp.float32
        dma = pltpu.SemaphoreType.DMA
        dims = (mats, tokens, d, ff)
        whole = jax.ShapeDtypeStruct((mats, d, ff), bf16)
        hbm = pl.BlockSpec(memory_space=pl.ANY)
        summed, later = pl.pallas_call(
            functools.partial(kernel, dims),
            out_shape=(jax.ShapeDtypeStruct((steps, ROWS, COLS), bf16), jax.ShapeDtypeStruct((steps // 2, eighth, COLS), bf16)),
            in_specs=[pl.BlockSpec(memory_space=pl.ANY)] * 2,
            out_specs=(hbm, hbm),
            scratch_shapes=[
                pltpu.VMEM((2, tokens, d), bf16),
                pltpu.VMEM((2, tokens, COLS), bf16),
                pltpu.VMEM((2, half, COLS), bf16),
                pltpu.VMEM((2, half, COLS), f32),
                pltpu.VMEM((2, half, COLS), bf16),
                pltpu.VMEM((RING_ONE, quarter, COLS), bf16),
                pltpu.VMEM((OWN_ONE, quarter, COLS), f32),
                pltpu.VMEM((RING_ONE, quarter, COLS), bf16),
                pltpu.VMEM((RING_TWO, eighth, COLS), bf16),
                pltpu.VMEM((OWN_TWO, eighth, COLS), f32),
                pltpu.VMEM((RING_TWO, eighth, COLS), bf16),
                pltpu.VMEM((steps, eighth, COLS), bf16),
                dma((2, d // ROWS)),
                dma((2,)),
                dma((2,)),
                dma((2,)),
                dma((RING_ONE,)),
                dma((RING_ONE,)),
                dma((RING_TWO,)),
                dma((RING_TWO,)),
            ]
            + [dma((steps,))] * 9
            + [dma((steps // 2,))] * 2
            + [dma((2, PIECES))],
            compiler_params=pltpu.CompilerParams(
                collective_id=0, has_side_effects=True, vmem_limit_bytes=VMEM_LIMIT
            ),
        )(a, g)

        opposite = lax.ppermute(later, "dp", [(i, i ^ (2 if i % 2 else 4)) for i in range(8)])
        result = pl.pallas_call(
            functools.partial(copy_kernel, dims),
            out_shape=whole,
            in_specs=[hbm],
            out_specs=hbm,
            scratch_shapes=[pltpu.VMEM((COPY_SLOTS, ROWS, COLS), bf16), dma((COPY_SLOTS,)), dma((COPY_SLOTS,))],
            compiler_params=pltpu.CompilerParams(vmem_limit_bytes=50 * 2**20),
            cost_estimate=pl.CostEstimate(flops=2 * 10**9, bytes_accessed=4 * mats * d * ff, transcendentals=0),
            name="copy",
        )(summed)

        def put(result, *sources_and_starts):
            sources, starts = sources_and_starts[::2], sources_and_starts[1::2]
            return pl.pallas_call(
                functools.partial(put_kernel, dims, starts),
                out_shape=whole,
                in_specs=[hbm] * (len(sources) + 1),
                out_specs=hbm,
                scratch_shapes=[dma((len(sources), steps // 2))],
                input_output_aliases={len(sources): 0},
                compiler_params=pltpu.CompilerParams(vmem_limit_bytes=16 * 2**20),
                cost_estimate=pl.CostEstimate(flops=2 * 10**8, bytes_accessed=4 * len(sources) * later.size, transcendentals=0),
                name="put",
            )(*sources, result)

        opposite, result = lax.optimization_barrier((opposite, result))
        mates = lax.ppermute(opposite, "dp", [(i, i ^ 1) for i in range(8)])
        result = put(result, later, there_of, opposite, opposite_of)
        return put(result, mates, mates_opposite_of)

    return jax.shard_map(
        step,
        mesh=mesh,
        in_specs=(P(("rep", "dp")), P(("rep", "dp"))),
        out_specs=P("rep"),
        check_vma=False,
    )
```
